32 devices in a mesh: dp: 4 (over y, x), rep: 8 (over z, core).
Axes of the slice: x: 2, y: 2, z: 4, core: 2. Of those that a mesh axis runs over, the one named last changes fastest.
Arguments:
- queries: bfloat16 [16384, 2048], P(('dp', 'rep')), may hold values from -32 to 32
- key_rows: bfloat16 [16384, 2048], P(('dp', 'rep')), may hold values from -32 to 32
- values: bfloat16 [16384, 2048], P(('dp', 'rep')), may hold values from -6 to 6
- upstream: bfloat16 [16384, 2048], P(('dp', 'rep')), may hold values from -6 to 6
- out_weight: bfloat16 [2048, 2048], P(('dp', 'rep')), may hold values from -0.125 to 0.125
- sample_ids: int32 [32, 512], P(('dp', 'rep')), may hold values from 0 to 3, as said below
Outputs:
- grad_queries: bfloat16 [16384, 2048], P(('dp', 'rep'))
- grad_keys: bfloat16 [16384, 2048], P(('dp', 'rep'))
- grad_values: bfloat16 [16384, 2048], P(('dp', 'rep'))
- grad_weight: float32 [2048, 2048], P(('dp', 'rep'))
The draws below stay inside these ranges and needn't reach their ends.
Inputs may be any that keep to these rules, and one draw needn't show every extreme that they name: `sample_ids`: within a row the ids never fall, every row starts with 0 and ends with 3, and the tokens of one sample are contiguous.
All inputs are finite; a program needn't handle non-finite values.
Results may differ from the reference program's by a relative error of at most 0.015.
Values may be sent and summed in bfloat16 or wider, within the bound.
A program may use at most 192 MiB of HBM per device.

```python
import math
import jax
import jax.numpy as jnp
from jax import lax

D = 2048
H = 16
DH = 128
HD = 2048
LEN = 512
NSEG = 4
SEQS = 32
TOKENS = 16384


def draw_queries(key, part):
    normal_part = jnp.clip(jax.random.normal(jax.random.fold_in(key, 11), (SEQS, LEN, H, DH), jnp.float32), -4.0, 4.0)
    normal_part = jnp.clip(normal_part, -32.0, 32.0)
    return normal_part.reshape(SEQS * LEN, H * DH).astype(jnp.bfloat16)


def draw_key_rows(key, part):
    normal_part = jnp.clip(jax.random.normal(jax.random.fold_in(key, 17), (SEQS, LEN, H, DH), jnp.float32), -4.0, 4.0)
    normal_part = jnp.clip(normal_part, -32.0, 32.0)
    return normal_part.reshape(SEQS * LEN, H * DH).astype(jnp.bfloat16)


def draw_sample_ids(key, part):
    cut_points = jax.random.randint(jax.random.fold_in(key, 29), (SEQS, NSEG - 1), LEN // 8, LEN - LEN // 8)
    positions = jnp.arange(LEN, dtype=jnp.int32)
    passed = (positions[None, :, None] >= cut_points[:, None, :]).astype(jnp.int32)
    return jnp.sum(passed, axis=2).astype(jnp.int32)


def with_spikes(array, own_key, source, target, parts, factor):
    def block_of(axis_at):
        return (jnp.arange(array.shape[axis_at]) // (array.shape[axis_at] // parts)).reshape((-1,) + (1,) * (array.ndim - 1 - axis_at))

    first = jax.random.permutation(own_key, parts)[block_of(target)]
    second = (block_of(target) + parts // 2) % parts
    return jnp.where((block_of(source) == first) | (block_of(source) == second), factor * array, array)


def shard_levels(rng, extent, shards, smallest, largest):
    level = 1.0
    for axis_at, parts in shards:
        draws = jax.random.uniform(jax.random.fold_in(jax.random.fold_in(rng, 6), axis_at), (parts,), jnp.float32, smallest / len(shards), largest / len(shards))
        level = level * jnp.repeat(jnp.exp(draws), extent[axis_at] // parts).reshape((-1,) + (1,) * (len(extent) - 1 - axis_at))
    return level


def bell_draw(stream_key, shape, scale, most, cuts=(), kind=jnp.bfloat16):
    result = scale * jax.random.normal(stream_key, shape, jnp.float32)
    if cuts:
        result = result * shard_levels(stream_key, shape, cuts, -0.22, 0.18)
    return jnp.clip(result, -most, most).astype(kind)


def gaussian_with(stream_key, extent, deviation, limit, pieces, heavy, kind=jnp.bfloat16):
    values = deviation * jax.random.normal(stream_key, extent, jnp.float32)
    if pieces:
        values = values * shard_levels(stream_key, extent, pieces, -0.22, 0.18)
    return jnp.clip(with_spikes(values, jax.random.fold_in(stream_key, 3), *heavy), -limit, limit).astype(kind)


def setup_inputs(seed: int = 0) -> dict:
    streams_of = jax.random.split(jax.random.key(seed), 7)
    return {
        "queries": draw_queries(jax.random.fold_in(streams_of[6], 71), 0),
        "key_rows": draw_key_rows(jax.random.fold_in(streams_of[6], 71), 0),
        "values": bell_draw(streams_of[2], (TOKENS, HD), 1.0, 6.0, ((0, 32),)),
        "upstream": gaussian_with(streams_of[3], (TOKENS, D), 1.0, 6.0, ((0, 32),), (0, 1, 32, 2.75)),
        "out_weight": bell_draw(streams_of[4], (D, HD), HD ** -0.5, 0.125, ((0, 32),)),
        "sample_ids": draw_sample_ids(jax.random.fold_in(streams_of[6], 71), 0),
    }


def sequence_pass(seq_block):
    query_block, key_block, value_block, grad_block, ids_row = seq_block
    scaling = 1.0 / math.sqrt(DH)
    query_wide = query_block.astype(jnp.float32)
    key_wide = key_block.astype(jnp.float32)
    value_wide = value_block.astype(jnp.float32)
    grad_wide = grad_block.astype(jnp.float32)
    positions = jnp.arange(LEN, dtype=jnp.int32)
    causal = positions[None, :] <= positions[:, None]
    allowed = jnp.logical_and(causal, ids_row[None, :] == ids_row[:, None])[None]
    scores = jnp.einsum('qhd,khd->hqk', query_wide, key_wide) * scaling
    masked = jnp.where(allowed, scores, -jnp.inf)
    row_max = lax.optimization_barrier(jnp.max(masked, axis=2, keepdims=True))
    raised = jnp.where(allowed, jnp.exp(masked - row_max), 0.0)
    probabilities = raised / lax.optimization_barrier(jnp.sum(raised, axis=2, keepdims=True))
    probs_low = lax.optimization_barrier(probabilities.astype(jnp.bfloat16)).astype(jnp.float32)
    attended = jnp.einsum('hqk,khd->qhd', probs_low, value_wide).astype(jnp.bfloat16)
    grad_values = jnp.einsum('hqk,qhd->khd', probs_low, grad_wide).astype(jnp.bfloat16)
    grad_probs = jnp.einsum('qhd,khd->hqk', grad_wide, value_wide)
    row_inner = lax.optimization_barrier(jnp.sum(probabilities * grad_probs, axis=2, keepdims=True))
    grad_scores = lax.optimization_barrier((probabilities * (grad_probs - row_inner)).astype(jnp.bfloat16)).astype(jnp.float32)
    grad_queries = (scaling * jnp.einsum('hqk,khd->qhd', grad_scores, key_wide)).astype(jnp.bfloat16)
    grad_keys = (scaling * jnp.einsum('hqk,qhd->khd', grad_scores, query_wide)).astype(jnp.bfloat16)
    return (attended, grad_queries, grad_keys, grad_values)

def reference(queries, key_rows, values, upstream, out_weight, sample_ids):
    grad_attended = jnp.dot(upstream, out_weight, preferred_element_type=jnp.float32).astype(jnp.bfloat16)
    grad_attended = lax.optimization_barrier(grad_attended)
    split_shape = (SEQS, LEN, H, DH)
    results = lax.map(sequence_pass, (queries.reshape(split_shape), key_rows.reshape(split_shape), values.reshape(split_shape), grad_attended.reshape(split_shape), sample_ids))
    attended, grad_queries, grad_keys, grad_values = [stacked.reshape(TOKENS, H * DH) for stacked in results]
    grad_weight = jnp.dot(upstream.T, attended, preferred_element_type=jnp.float32) / math.sqrt(TOKENS)
    return (grad_queries, grad_keys, grad_values, grad_weight)
```

```python
import functools
import math

import jax
import jax.numpy as jnp
from jax import lax
from jax.experimental import pallas as pl
from jax.experimental.pallas import tpu as pltpu
from jax.sharding import PartitionSpec as P

DH = 128
MESH = pl.DeviceIdType.MESH
F32 = jnp.float32
BF16 = jnp.bfloat16
SCALING = 1.0 / math.sqrt(DH)
VMEM_LIMIT = 60 * 1024 * 1024


def dot_nt(a, b):
    return lax.dot_general(a, b, (((1,), (1,)), ((), ())), preferred_element_type=F32)


def dot_tn(a, b):
    return lax.dot_general(a, b, (((0,), (0,)), ((), ())), preferred_element_type=F32)


def dot_nn(a, b):
    return jnp.dot(a, b, preferred_element_type=F32)


def fill_bias(bias, ids_row, ids_col):
    size = bias.shape[0]
    rows = lax.broadcasted_iota(jnp.int32, (size, size), 0)
    cols = lax.broadcasted_iota(jnp.int32, (size, size), 1)
    allowed = jnp.logical_and(cols <= rows, ids_row[...] == ids_col[...])
    bias[...] = jnp.where(allowed, 0.0, -1e30).astype(F32)


def block_probs(q, k, bias):
    s = dot_nt(q, k) + bias
    e = jnp.exp((s - jnp.max(s, axis=1, keepdims=True)) * SCALING)
    return e * (1.0 / jnp.sum(e, axis=1, keepdims=True))


def head_forward(q_ref, k_ref, v_ref, o_ref, bias, cols):
    size = bias.shape[0]
    half = size // 2
    for at in range(2):
        rows, end = pl.ds(at * half, half), pl.ds(0, (at + 1) * half)
        p = block_probs(q_ref[rows, cols], k_ref[end, cols], bias[rows, end]).astype(BF16)
        o_ref[rows, cols] = dot_nn(p, v_ref[end, cols]).astype(BF16)


def head_backward(q_ref, k_ref, v_ref, g_ref, dq_ref, dk_ref, dv_ref, bias, cols):
    size = bias.shape[0]
    half = size // 2
    grads = []
    for at in range(2):
        rows, end = pl.ds(at * half, half), pl.ds(0, (at + 1) * half)
        q, k, v, g = q_ref[rows, cols], k_ref[end, cols], v_ref[end, cols], g_ref[rows, cols]
        p = block_probs(q, k, bias[rows, end])
        dv = dot_tn(p.astype(BF16), g)
        dp = dot_nt(g, v)
        inner = jnp.sum(p * dp, axis=1, keepdims=True)
        ds = (p * (dp - inner)).astype(BF16)
        dq_ref[rows, cols] = (dot_nn(ds, k) * SCALING).astype(BF16)
        grads.append((dot_tn(ds, q), dv))
    (dk0, dv0), (dk1, dv1) = grads
    top, low = pl.ds(0, half), pl.ds(half, half)
    dk_ref[top, cols] = ((dk0 + dk1[:half]) * SCALING).astype(BF16)
    dk_ref[low, cols] = (dk1[half:] * SCALING).astype(BF16)
    dv_ref[top, cols] = (dv0 + dv1[:half]).astype(BF16)
    dv_ref[low, cols] = dv1[half:].astype(BF16)


def forward_kernel(row_ref, col_ref, q_ref, k_ref, v_ref, o_ref, bias):
    @pl.when(pl.program_id(0) == 0)
    def _():
        fill_bias(bias, row_ref, col_ref)

    head_forward(q_ref, k_ref, v_ref, o_ref, bias, pl.ds(0, DH))


def backward_kernel(row_ref, col_ref, q_ref, k_ref, v_ref, g_ref, dq_ref, dk_ref, dv_ref, bias):
    @pl.when(pl.program_id(0) == 0)
    def _():
        fill_bias(bias, row_ref, col_ref)

    head_backward(
        q_ref, k_ref, v_ref, g_ref, dq_ref, dk_ref, dv_ref, bias, pl.ds(0, DH)
    )


def attention_call(kernel, ids, arrays, outs, flops):
    size = ids.shape[1]
    heads = arrays[0].shape[1] // DH
    block = pl.BlockSpec((size, DH), lambda h: (0, h))
    whole = [
        pl.BlockSpec((1, size), lambda h: (0, 0)),
        pl.BlockSpec((size, 1), lambda h: (0, 0)),
    ]
    result = pl.pallas_call(
        kernel,
        grid=(heads,),
        out_shape=[jax.ShapeDtypeStruct(arrays[0].shape, BF16)] * outs,
        in_specs=whole + [block] * len(arrays),
        out_specs=[block] * outs,
        scratch_shapes=[pltpu.VMEM((size, size), F32)],
        compiler_params=pltpu.CompilerParams(dimension_semantics=("arbitrary",)),
        cost_estimate=pl.CostEstimate(
            flops=flops * 2 * size * size * DH * heads,
            bytes_accessed=2 * size * DH * heads * (len(arrays) + outs),
            transcendentals=size * size * heads,
        ),
    )(ids, ids.reshape(size, 1), *arrays)
    return result


class Place:
    def __init__(self, n_rep):
        self.n_rep = n_rep
        self.line = n_rep // 2
        self.dp = lax.axis_index("dp")
        rep = lax.axis_index("rep")
        self.r = rep // 2
        self.c = rep % 2

    def across(self, bit):
        return self.dp + bit - 2 * bit * ((self.dp // bit) % 2)

    def shard(self, dp, r, c):
        return dp * self.n_rep + r * 2 + c

    def dev(self, dp, r, c):
        return (dp, r * 2 + c)

    def greet(self):
        barrier = pltpu.get_barrier_semaphore()

        def signal(dev):
            pl.semaphore_signal(barrier, inc=1, device_id=dev, device_id_type=MESH)

        for bit in (1, 2):
            signal(self.dev(self.across(bit), self.r, self.c))
        signal(self.dev(self.dp, self.r, 1 - self.c))

        @pl.when(self.r > 0)
        def _():
            signal(self.dev(self.dp, self.r - 1, self.c))

        @pl.when(self.r < self.line - 1)
        def _():
            signal(self.dev(self.dp, self.r + 1, self.c))

        inner = jnp.logical_and(self.r > 0, self.r < self.line - 1)

        @pl.when(inner)
        def _():
            pl.semaphore_wait(barrier, 5)

        @pl.when(jnp.logical_not(inner))
        def _():
            pl.semaphore_wait(barrier, 4 if self.line > 1 else 3)


def rcopy(src, dst, send, recv, dev):
    return pltpu.make_async_remote_copy(
        src_ref=src, dst_ref=dst, send_sem=send, recv_sem=recv, device_id=dev, device_id_type=MESH
    )


def gather_events(n_rep, w_ref, all_ref, zs, zr, ps, pr, cs, cr, own_sem):
    me = Place(n_rep)
    depth = w_ref.shape[0]
    half = depth // 2
    line = me.line
    order = ((1, 2), (2, 1))

    def rows(dp, r, c, piece=None):
        start = pl.multiple_of(me.shard(dp, r, c) * depth, depth)
        if piece is None:
            return all_ref.at[pl.ds(start, depth)]
        return all_ref.at[pl.ds(pl.multiple_of(start + piece * half, half), half)]

    def zcopy(s, up):
        to = me.r + (1 if up else -1)
        ref = rows(me.dp, s, me.c)
        return rcopy(ref, ref, zs.at[1 if up else 0, s], zr.at[s], me.dev(me.dp, to, me.c))

    def zrecv(s):
        ref = rows(me.dp, s, me.c)
        rcopy(ref, ref, zs.at[0, s], zr.at[s], me.dev(me.dp, me.r, 1 - me.c)).wait_recv()

    def pcopy(dp, s, piece, step):
        bit = order[piece][step]
        ref = rows(dp, s, me.c, piece)
        return rcopy(
            ref, ref, ps.at[dp, s, 2 * piece + step], pr.at[dp, s, piece],
            me.dev(me.across(bit), me.r, me.c),
        )

    def ccopy(dp, s, piece):
        ref = rows(dp, s, me.c, piece)
        return rcopy(
            ref, ref, cs.at[dp, s, piece], cr.at[dp, s, piece], me.dev(me.dp, me.r, 1 - me.c)
        )

    def crecv(dp, s, piece):
        ref = rows(dp, s, 1 - me.c, piece)
        rcopy(
            ref, ref, cs.at[dp, s, piece], cr.at[dp, s, piece], me.dev(me.dp, me.r, 1 - me.c)
        ).wait_recv()

    def first():
        own = pltpu.make_async_copy(w_ref, rows(me.dp, me.r, me.c), own_sem)
        own.start()
        me.greet()
        own.wait()

        @pl.when(me.r < line - 1)
        def _():
            zcopy(me.r, True).start()

        @pl.when(me.r > 0)
        def _():
            zcopy(me.r, False).start()

        spread(me.r)

    def spread(s):
        for piece in range(2):
            pcopy(me.dp, s, piece, 0).start()
        for piece in range(2):
            pcopy(me.dp, s, piece, 1).start()
        for piece in range(2):
            ccopy(me.dp, s, piece).start()

    def relay(s):
        for piece in range(2):
            src = me.across(order[piece][0])
            pcopy(src, s, piece, 0).wait_recv()
            pcopy(src, s, piece, 1).start()
            ccopy(src, s, piece).start()

    def last(s):
        for piece in range(2):
            near = me.across(order[piece][1])
            for dp in (near, 3 - me.dp):
                pcopy(dp, s, piece, 0).wait_recv()
                ccopy(dp, s, piece).start()

    def drain(s):
        for piece in range(2):
            near0 = me.across(order[piece][0])
            pcopy(me.dp, s, piece, 0).wait_send()
            pcopy(me.dp, s, piece, 1).wait_send()
            pcopy(near0, s, piece, 1).wait_send()
            for dp in (me.dp, me.across(1), me.across(2), 3 - me.dp):
                ccopy(dp, s, piece).wait_send()
                crecv(dp, s, piece)

    def each(d, act):
        if d == 0:
            act(me.r, 0)
            return

        @pl.when(me.r >= d)
        def _():
            act(me.r - d, 1)

        @pl.when(me.r + d < line)
        def _():
            act(me.r + d, -1)

    def arrive(s, side):
        zrecv(s)
        if side == 1:

            @pl.when(me.r < line - 1)
            def _():
                zcopy(s, True).start()

        else:

            @pl.when(me.r > 0)
            def _():
                zcopy(s, False).start()

        spread(s)

    def zdrain(s, side):
        if side >= 0:

            @pl.when(me.r < line - 1)
            def _():
                zcopy(s, True).wait_send()

        if side <= 0:

            @pl.when(me.r > 0)
            def _():
                zcopy(s, False).wait_send()

    events = [first]
    for d in range(line):
        events.append(lambda d=d: each(d, lambda s, side: relay(s)))
        if d + 1 < line:
            events.append(lambda d=d: each(d + 1, arrive))
        events.append(lambda d=d: each(d, lambda s, side: last(s)))

    def finish():
        for d in range(line):
            each(d, lambda s, side: drain(s))
            each(d, zdrain)

    events.append(finish)
    return events


def gather_scratch(n_dp, n_rep):
    line = n_rep // 2
    dma = pltpu.SemaphoreType.DMA
    return [
        dma((2, line)), dma((line,)),
        dma((n_dp, line, 4)), dma((n_dp, line, 2)),
        dma((n_dp, line, 2)), dma((n_dp, line, 2)),
        dma,
    ]


def gather_kernel(n_rep, w_ref, all_ref, *sems):
    for event in gather_events(n_rep, w_ref, all_ref, *sems):
        event()


def gather_weight(w, n_dp, n_rep):
    vm = pl.BlockSpec(memory_space=pltpu.VMEM)
    return pl.pallas_call(
        functools.partial(gather_kernel, n_rep),
        out_shape=jax.ShapeDtypeStruct((n_dp * n_rep * w.shape[0], w.shape[1]), w.dtype),
        in_specs=[vm],
        out_specs=vm,
        scratch_shapes=gather_scratch(n_dp, n_rep),
        compiler_params=pltpu.CompilerParams(
            collective_id=0, has_side_effects=True, vmem_limit_bytes=VMEM_LIMIT
        ),
    )(w)


def shards(queries, key_rows, values, upstream, out_weight, sample_ids):
    n_dp, n_rep = lax.axis_size("dp"), lax.axis_size("rep")
    total_tokens = queries.shape[0] * n_dp * n_rep
    square = n_dp == 4 and n_rep % 2 == 0
    qkv = (queries, key_rows, values)
    (attended,) = attention_call(forward_kernel, sample_ids, qkv, 1, 2)
    part = lax.dot_general(
        upstream, attended, (((0,), (0,)), ((), ())), preferred_element_type=F32
    ).astype(BF16)
    group_sums = lax.psum_scatter(part, "dp", scatter_dimension=0, tiled=True)
    summed = lax.psum_scatter(group_sums, "rep", scatter_dimension=0, tiled=True)
    grad_weight = summed.astype(F32) * (1.0 / math.sqrt(total_tokens))
    if square:
        weight = gather_weight(out_weight, n_dp, n_rep)
    else:
        weight = lax.all_gather(out_weight, ("dp", "rep"), axis=0, tiled=True)
    grad_attended = jnp.dot(upstream, weight, preferred_element_type=F32).astype(BF16)
    grads = attention_call(backward_kernel, sample_ids, qkv + (grad_attended,), 3, 5)
    return (*grads, grad_weight)


def solution(mesh):
    spec = P(("dp", "rep"), None)
    return jax.shard_map(
        shards, mesh=mesh, in_specs=(spec,) * 6, out_specs=(spec,) * 4, check_vma=False
    )
```

```python
import functools
import math

import jax
import jax.numpy as jnp
from jax import lax
from jax.experimental import pallas as pl
from jax.experimental.pallas import tpu as pltpu
from jax.sharding import PartitionSpec as P

DH = 128
MESH = pl.DeviceIdType.MESH
F32 = jnp.float32
BF16 = jnp.bfloat16
SCALING = 1.0 / math.sqrt(DH)
VMEM_LIMIT = 60 * 1024 * 1024


def dot_nt(a, b):
    return lax.dot_general(a, b, (((1,), (1,)), ((), ())), preferred_element_type=F32)


def dot_tn(a, b):
    return lax.dot_general(a, b, (((0,), (0,)), ((), ())), preferred_element_type=F32)


def dot_nn(a, b):
    return jnp.dot(a, b, preferred_element_type=F32)


def fill_bias(bias, ids_row, ids_col):
    size = bias.shape[0]
    rows = lax.broadcasted_iota(jnp.int32, (size, size), 0)
    cols = lax.broadcasted_iota(jnp.int32, (size, size), 1)
    allowed = jnp.logical_and(cols <= rows, ids_row[...] == ids_col[...])
    bias[...] = jnp.where(allowed, 0.0, -1e30).astype(F32)


def block_probs(q, k, bias):
    s = dot_nt(q, k) + bias
    e = jnp.exp((s - jnp.max(s, axis=1, keepdims=True)) * SCALING)
    return e * (1.0 / jnp.sum(e, axis=1, keepdims=True))


def head_forward(q_ref, k_ref, v_ref, o_ref, bias, cols):
    size = bias.shape[0]
    half = size // 2
    for at in range(2):
        rows, end = pl.ds(at * half, half), pl.ds(0, (at + 1) * half)
        p = block_probs(q_ref[rows, cols], k_ref[end, cols], bias[rows, end]).astype(BF16)
        o_ref[rows, cols] = dot_nn(p, v_ref[end, cols]).astype(BF16)


def head_backward(q_ref, k_ref, v_ref, g_ref, dq_ref, dk_ref, dv_ref, bias, cols):
    size = bias.shape[0]
    half = size // 2
    grads = []
    for at in range(2):
        rows, end = pl.ds(at * half, half), pl.ds(0, (at + 1) * half)
        q, k, v, g = q_ref[rows, cols], k_ref[end, cols], v_ref[end, cols], g_ref[rows, cols]
        p = block_probs(q, k, bias[rows, end])
        dv = dot_tn(p.astype(BF16), g)
        dp = dot_nt(g, v)
        inner = jnp.sum(p * dp, axis=1, keepdims=True)
        ds = (p * (dp - inner)).astype(BF16)
        dq_ref[rows, cols] = (dot_nn(ds, k) * SCALING).astype(BF16)
        grads.append((dot_tn(ds, q), dv))
    (dk0, dv0), (dk1, dv1) = grads
    top, low = pl.ds(0, half), pl.ds(half, half)
    dk_ref[top, cols] = ((dk0 + dk1[:half]) * SCALING).astype(BF16)
    dk_ref[low, cols] = (dk1[half:] * SCALING).astype(BF16)
    dv_ref[top, cols] = (dv0 + dv1[:half]).astype(BF16)
    dv_ref[low, cols] = dv1[half:].astype(BF16)


def forward_kernel(row_ref, col_ref, q_ref, k_ref, v_ref, o_ref, bias):
    @pl.when(pl.program_id(0) == 0)
    def _():
        fill_bias(bias, row_ref, col_ref)

    head_forward(q_ref, k_ref, v_ref, o_ref, bias, pl.ds(0, DH))


def backward_kernel(row_ref, col_ref, q_ref, k_ref, v_ref, g_ref, dq_ref, dk_ref, dv_ref, bias):
    @pl.when(pl.program_id(0) == 0)
    def _():
        fill_bias(bias, row_ref, col_ref)

    head_backward(
        q_ref, k_ref, v_ref, g_ref, dq_ref, dk_ref, dv_ref, bias, pl.ds(0, DH)
    )


def attention_call(kernel, ids, arrays, outs, flops):
    size = ids.shape[1]
    heads = arrays[0].shape[1] // DH
    block = pl.BlockSpec((size, DH), lambda h: (0, h))
    whole = [
        pl.BlockSpec((1, size), lambda h: (0, 0)),
        pl.BlockSpec((size, 1), lambda h: (0, 0)),
    ]
    result = pl.pallas_call(
        kernel,
        grid=(heads,),
        out_shape=[jax.ShapeDtypeStruct(arrays[0].shape, BF16)] * outs,
        in_specs=whole + [block] * len(arrays),
        out_specs=[block] * outs,
        scratch_shapes=[pltpu.VMEM((size, size), F32)],
        compiler_params=pltpu.CompilerParams(dimension_semantics=("arbitrary",)),
        cost_estimate=pl.CostEstimate(
            flops=flops * 2 * size * size * DH * heads,
            bytes_accessed=2 * size * DH * heads * (len(arrays) + outs),
            transcendentals=size * size * heads,
        ),
    )(ids, ids.reshape(size, 1), *arrays)
    return result


class Place:
    def __init__(self, n_rep):
        self.n_rep = n_rep
        self.line = n_rep // 2
        self.dp = lax.axis_index("dp")
        rep = lax.axis_index("rep")
        self.r = rep // 2
        self.c = rep % 2

    def across(self, bit):
        return self.dp + bit - 2 * bit * ((self.dp // bit) % 2)

    def shard(self, dp, r, c):
        return dp * self.n_rep + r * 2 + c

    def dev(self, dp, r, c):
        return (dp, r * 2 + c)

    def greet(self):
        barrier = pltpu.get_barrier_semaphore()

        def signal(dev):
            pl.semaphore_signal(barrier, inc=1, device_id=dev, device_id_type=MESH)

        for bit in (1, 2):
            signal(self.dev(self.across(bit), self.r, self.c))
        signal(self.dev(self.dp, self.r, 1 - self.c))

        @pl.when(self.r > 0)
        def _():
            signal(self.dev(self.dp, self.r - 1, self.c))

        @pl.when(self.r < self.line - 1)
        def _():
            signal(self.dev(self.dp, self.r + 1, self.c))

        inner = jnp.logical_and(self.r > 0, self.r < self.line - 1)

        @pl.when(inner)
        def _():
            pl.semaphore_wait(barrier, 5)

        @pl.when(jnp.logical_not(inner))
        def _():
            pl.semaphore_wait(barrier, 4 if self.line > 1 else 3)


def rcopy(src, dst, send, recv, dev):
    return pltpu.make_async_remote_copy(
        src_ref=src, dst_ref=dst, send_sem=send, recv_sem=recv, device_id=dev, device_id_type=MESH
    )


def gather_events(n_rep, w_ref, all_ref, zs, zr, ps, pr, cs, cr, own_sem):
    me = Place(n_rep)
    depth = w_ref.shape[0]
    half = depth // 2
    line = me.line
    order = ((1, 2), (2, 1))

    def rows(dp, r, c, piece=None):
        start = pl.multiple_of(me.shard(dp, r, c) * depth, depth)
        if piece is None:
            return all_ref.at[pl.ds(start, depth)]
        return all_ref.at[pl.ds(pl.multiple_of(start + piece * half, half), half)]

    def zcopy(s, up):
        to = me.r + (1 if up else -1)
        ref = rows(me.dp, s, me.c)
        return rcopy(ref, ref, zs.at[1 if up else 0, s], zr.at[s], me.dev(me.dp, to, me.c))

    def zrecv(s):
        ref = rows(me.dp, s, me.c)
        rcopy(ref, ref, zs.at[0, s], zr.at[s], me.dev(me.dp, me.r, 1 - me.c)).wait_recv()

    def pcopy(dp, s, piece, step):
        bit = order[piece][step]
        ref = rows(dp, s, me.c, piece)
        return rcopy(
            ref, ref, ps.at[dp, s, 2 * piece + step], pr.at[dp, s, piece],
            me.dev(me.across(bit), me.r, me.c),
        )

    def ccopy(dp, s, piece):
        ref = rows(dp, s, me.c, piece)
        return rcopy(
            ref, ref, cs.at[dp, s, piece], cr.at[dp, s, piece], me.dev(me.dp, me.r, 1 - me.c)
        )

    def crecv(dp, s, piece):
        ref = rows(dp, s, 1 - me.c, piece)
        rcopy(
            ref, ref, cs.at[dp, s, piece], cr.at[dp, s, piece], me.dev(me.dp, me.r, 1 - me.c)
        ).wait_recv()

    def first():
        own = pltpu.make_async_copy(w_ref, rows(me.dp, me.r, me.c), own_sem)
        own.start()
        me.greet()
        own.wait()

        @pl.when(me.r < line - 1)
        def _():
            zcopy(me.r, True).start()

        @pl.when(me.r > 0)
        def _():
            zcopy(me.r, False).start()

        spread(me.r)

    def spread(s):
        for piece in range(2):
            pcopy(me.dp, s, piece, 0).start()
        for piece in range(2):
            pcopy(me.dp, s, piece, 1).start()
        for piece in range(2):
            ccopy(me.dp, s, piece).start()

    def relay(s):
        for piece in range(2):
            src = me.across(order[piece][0])
            pcopy(src, s, piece, 0).wait_recv()
            pcopy(src, s, piece, 1).start()
            ccopy(src, s, piece).start()

    def last(s):
        for piece in range(2):
            near = me.across(order[piece][1])
            for dp in (near, 3 - me.dp):
                pcopy(dp, s, piece, 0).wait_recv()
                ccopy(dp, s, piece).start()

    def drain(s):
        for piece in range(2):
            near0 = me.across(order[piece][0])
            pcopy(me.dp, s, piece, 0).wait_send()
            pcopy(me.dp, s, piece, 1).wait_send()
            pcopy(near0, s, piece, 1).wait_send()
            for dp in (me.dp, me.across(1), me.across(2), 3 - me.dp):
                ccopy(dp, s, piece).wait_send()
                crecv(dp, s, piece)

    def each(d, act):
        if d == 0:
            act(me.r, 0)
            return

        @pl.when(me.r >= d)
        def _():
            act(me.r - d, 1)

        @pl.when(me.r + d < line)
        def _():
            act(me.r + d, -1)

    def arrive(s, side):
        zrecv(s)
        if side == 1:

            @pl.when(me.r < line - 1)
            def _():
                zcopy(s, True).start()

        else:

            @pl.when(me.r > 0)
            def _():
                zcopy(s, False).start()

        spread(s)

    def zdrain(s, side):
        if side >= 0:

            @pl.when(me.r < line - 1)
            def _():
                zcopy(s, True).wait_send()

        if side <= 0:

            @pl.when(me.r > 0)
            def _():
                zcopy(s, False).wait_send()

    events = [first]
    for d in range(line):
        events.append(lambda d=d: each(d, lambda s, side: relay(s)))
        if d + 1 < line:
            events.append(lambda d=d: each(d + 1, arrive))
        events.append(lambda d=d: each(d, lambda s, side: last(s)))

    def finish():
        for d in range(line):
            each(d, lambda s, side: drain(s))
            each(d, zdrain)

    events.append(finish)
    return events


def gather_scratch(n_dp, n_rep):
    line = n_rep // 2
    dma = pltpu.SemaphoreType.DMA
    return [
        dma((2, line)), dma((line,)),
        dma((n_dp, line, 4)), dma((n_dp, line, 2)),
        dma((n_dp, line, 2)), dma((n_dp, line, 2)),
        dma,
    ]


def interleave(events, work):
    left = list(work)
    for at, event in enumerate(events):
        event()
        if at < len(events) - 2:
            if left:
                left.pop(0)()
        elif at == len(events) - 2:
            for piece in left:
                piece()


def loop_work(begin, end, act):
    def run():
        lax.fori_loop(begin, end, lambda i, carry: (act(i), carry)[1], 0)

    return run


def head_cols(h):
    return pl.ds(pl.multiple_of(h * DH, DH), DH)


def gather_kernel(
    n_rep, w_ref, row_ref, col_ref, q_ref, k_ref, v_ref, up_ref, all_ref, part_ref,
    bias, att, *sems,
):
    heads = q_ref.shape[1] // DH
    blocks = up_ref.shape[1] // DH

    def head(h):
        head_forward(q_ref, k_ref, v_ref, att, bias, head_cols(h))

    def block(i):
        cols = head_cols(i)
        part_ref[cols, :] = dot_tn(up_ref[:, cols], att[...]).astype(BF16)

    events = gather_events(n_rep, w_ref, all_ref, *sems)
    work = [lambda: fill_bias(bias, row_ref, col_ref)]
    pieces = 6
    work += [
        loop_work(heads * i // pieces, heads * (i + 1) // pieces, head) for i in range(pieces)
    ]
    pieces = 4
    work += [
        loop_work(blocks * i // pieces, blocks * (i + 1) // pieces, block) for i in range(pieces)
    ]
    interleave(events, work)


def gather_weight(w, ids, qkv, upstream, n_dp, n_rep):
    vm = pl.BlockSpec(memory_space=pltpu.VMEM)
    size = ids.shape[1]
    width = qkv[0].shape[1]
    return pl.pallas_call(
        functools.partial(gather_kernel, n_rep),
        out_shape=[
            jax.ShapeDtypeStruct((n_dp * n_rep * w.shape[0], width), BF16),
            jax.ShapeDtypeStruct((upstream.shape[1], width), BF16),
        ],
        in_specs=[vm] * 7,
        out_specs=[vm] * 2,
        scratch_shapes=[
            pltpu.VMEM((size, size), F32), pltpu.VMEM((size, width), BF16),
            *gather_scratch(n_dp, n_rep),
        ],
        compiler_params=pltpu.CompilerParams(
            collective_id=0, has_side_effects=True, vmem_limit_bytes=VMEM_LIMIT
        ),
    )(w, ids, ids.reshape(size, 1), *qkv, upstream)


def scatter_events(
    n_dp, n_rep, scale, part_ref, out_ref, acc, got0, got1, got2, gotz,
    s0, r0, s1, r1, s2, r2, sz, rz,
):
    me = Place(n_rep)
    depth = out_ref.shape[0]
    half = depth // 2
    line = me.line
    order = ((1, 2), (2, 1))
    far = 3 - me.dp

    def prows(dp, s, c):
        return pl.ds(pl.multiple_of(me.shard(dp, s, c) * depth, depth), depth)

    def piece_rows(piece):
        return pl.ds(piece * half, half)

    def c0(dp, s):
        return rcopy(
            part_ref.at[prows(dp, s, 1 - me.c)], got0.at[dp, s], s0.at[dp, s], r0.at[dp, s],
            me.dev(me.dp, me.r, 1 - me.c),
        )

    def c1(s, piece, slot):
        near = me.across(order[piece][0])
        src = (near, far)[slot]
        return rcopy(
            acc.at[src, s, piece_rows(piece)], got1.at[s, piece, slot],
            s1.at[s, piece, slot], r1.at[s, piece, slot], me.dev(near, me.r, me.c),
        )

    def c2(s, piece):
        near = me.across(order[piece][1])
        return rcopy(
            acc.at[near, s, piece_rows(piece)], got2.at[s, piece],
            s2.at[s, piece], r2.at[s, piece], me.dev(near, me.r, me.c),
        )

    def cz(s, side, to):
        return rcopy(
            acc.at[me.dp, s], gotz.at[s, side], sz.at[s], rz.at[s, side], me.dev(me.dp, to, me.c)
        )

    def zwait(s, side):
        rcopy(
            acc.at[me.dp, s], gotz.at[s, side], sz.at[s], rz.at[s, side],
            me.dev(me.dp, me.r, 1 - me.c),
        ).wait_recv()

    def each(d, act):
        if d == 0:
            act(me.r, None)
            return

        @pl.when(me.r + d < line)
        def _():
            act(me.r + d, 0)

        @pl.when(me.r >= d)
        def _():
            act(me.r - d, 1)

    def first():
        me.greet()
        for d in reversed(range(line)):
            each(d, lambda s, side: [c0(dp, s).start() for dp in range(n_dp)] and None)

    def prep(s, side):
        for dp in range(n_dp):
            c0(dp, s).wait_recv()
            acc[dp, s] = (
                part_ref[prows(dp, s, me.c), :].astype(F32) + got0[dp, s].astype(F32)
            ).astype(BF16)
        for slot in (1, 0):
            for piece in range(2):
                c1(s, piece, slot).start()

    def mid(s, side):
        for piece in range(2):
            near = me.across(order[piece][1])
            for slot, dp in ((1, near), (0, me.dp)):
                c1(s, piece, slot).wait_recv()
                acc[dp, s, piece_rows(piece)] = (
                    acc[dp, s, piece_rows(piece)].astype(F32) + got1[s, piece, slot].astype(F32)
                ).astype(BF16)
                if slot == 1:
                    c2(s, piece).start()

    def fin(s, side):
        for piece in range(2):
            c2(s, piece).wait_recv()
            acc[me.dp, s, piece_rows(piece)] = (
                acc[me.dp, s, piece_rows(piece)].astype(F32) + got2[s, piece].astype(F32)
            ).astype(BF16)

        def add(at):
            acc[me.dp, s] = (acc[me.dp, s].astype(F32) + gotz[s, at].astype(F32)).astype(BF16)

        def from_below():
            @pl.when(me.r > 0)
            def _():
                zwait(s, 0)
                if side is None:
                    out_ref[...] += gotz[s, 0].astype(F32)
                else:
                    add(0)

        def from_above():
            @pl.when(me.r < line - 1)
            def _():
                zwait(s, 1)
                if side is None:
                    out_ref[...] += gotz[s, 1].astype(F32)
                else:
                    add(1)

        if side is None:
            out_ref[...] = acc[me.dp, s].astype(F32)
            from_below()
            from_above()
            out_ref[...] *= scale
        elif side == 0:
            from_below()
            cz(s, 0, me.r + 1).start()
        else:
            from_above()
            cz(s, 1, me.r - 1).start()

    def drain(s, side):
        for dp in range(n_dp):
            c0(dp, s).wait_send()
        for piece in range(2):
            for slot in range(2):
                c1(s, piece, slot).wait_send()
            c2(s, piece).wait_send()
        if side == 0:
            cz(s, 0, me.r + 1).wait_send()
        elif side == 1:
            cz(s, 1, me.r - 1).wait_send()

    def event(d, act):
        return lambda: each(d, act)

    events = [first]
    dists = list(reversed(range(line)))
    for at in range(line + 2):
        if at < line:
            events.append(event(dists[at], prep))
        if 0 <= at - 1 < line:
            events.append(event(dists[at - 1], mid))
        if 0 <= at - 2 < line:
            events.append(event(dists[at - 2], fin))

    def finish():
        for d in dists:
            each(d, drain)

    events.append(finish)
    return events


def scatter_scratch(n_dp, n_rep, depth, width):
    line = n_rep // 2
    half = depth // 2
    dma = pltpu.SemaphoreType.DMA
    return [
        pltpu.VMEM((n_dp, line, depth, width), BF16),
        pltpu.VMEM((n_dp, line, depth, width), BF16),
        pltpu.VMEM((line, 2, 2, half, width), BF16),
        pltpu.VMEM((line, 2, half, width), BF16),
        pltpu.VMEM((line, 2, depth, width), BF16),
        dma((n_dp, line)), dma((n_dp, line)),
        dma((line, 2, 2)), dma((line, 2, 2)),
        dma((line, 2)), dma((line, 2)),
        dma((line,)), dma((line, 2)),
    ]


def scatter_kernel(n_dp, n_rep, scale, part_ref, out_ref, *scratch):
    for event in scatter_events(n_dp, n_rep, scale, part_ref, out_ref, *scratch):
        event()


def scatter_grad(part, scale, n_dp, n_rep):
    vm = pl.BlockSpec(memory_space=pltpu.VMEM)
    depth = part.shape[0] // (n_dp * n_rep)
    return pl.pallas_call(
        functools.partial(scatter_kernel, n_dp, n_rep, scale),
        out_shape=jax.ShapeDtypeStruct((depth, part.shape[1]), F32),
        in_specs=[vm],
        out_specs=vm,
        scratch_shapes=scatter_scratch(n_dp, n_rep, depth, part.shape[1]),
        compiler_params=pltpu.CompilerParams(
            collective_id=1, has_side_effects=True, vmem_limit_bytes=VMEM_LIMIT
        ),
    )(part)


def shards(queries, key_rows, values, upstream, out_weight, sample_ids):
    n_dp, n_rep = lax.axis_size("dp"), lax.axis_size("rep")
    scale = 1.0 / math.sqrt(queries.shape[0] * n_dp * n_rep)
    qkv = (queries, key_rows, values)
    if n_dp == 4 and n_rep % 2 == 0:
        weight, part = gather_weight(out_weight, sample_ids, qkv, upstream, n_dp, n_rep)
        grad_weight = scatter_grad(part, scale, n_dp, n_rep)
    else:
        (attended,) = attention_call(forward_kernel, sample_ids, qkv, 1, 2)
        part = dot_tn(upstream, attended).astype(BF16)
        group_sums = lax.psum_scatter(part, "dp", scatter_dimension=0, tiled=True)
        summed = lax.psum_scatter(group_sums, "rep", scatter_dimension=0, tiled=True)
        grad_weight = summed.astype(F32) * scale
        weight = lax.all_gather(out_weight, ("dp", "rep"), axis=0, tiled=True)
    grad_attended = dot_nn(upstream, weight).astype(BF16)
    grads = attention_call(backward_kernel, sample_ids, qkv + (grad_attended,), 3, 5)
    return (*grads, grad_weight)


def solution(mesh):
    spec = P(("dp", "rep"), None)
    return jax.shard_map(
        shards, mesh=mesh, in_specs=(spec,) * 6, out_specs=(spec,) * 4, check_vma=False
    )
```
